32 devices in a mesh: groups: 2 (over y), ep: 4 (over z), tp: 4 (over x, core).
Axes of the slice: x: 2, y: 2, z: 4, core: 2. Of those that a mesh axis runs over, the one named last changes fastest.
Arguments:
- context: bfloat16 [512, 4096], P(('groups', 'ep'), 'tp'), parts along dimension 0, may hold values from -6 to 6
- stream: bfloat16 [512, 4096], P(('groups', 'ep'), 'tp'), parts along dimension 0, may hold values from -14 to 14
- out_proj: bfloat16 [4096, 4096], P('tp', 'ep'), may hold values from -0.09375 to 0.09375
- norm_gain: bfloat16 [4096], P('tp'), may hold values from 0.099609375 to 1.8984375
- router: bfloat16 [4096, 4], P('tp'), may hold values from -0.0625 to 0.0625
- expert_ids: int32 [512, 2], P(('groups', 'ep')), parts along dimension 0, may hold values from 0 to 3, all different within a row; in each aligned block of 64 rows (0 to 63, 64 to 127, ...) at most 36 rows name the same one
- w_gate: bfloat16 [4096, 28672], P('tp', 'ep'), may hold values from -0.09375 to 0.09375
- w_up: bfloat16 [4096, 28672], P('tp', 'ep'), may hold values from -0.09375 to 0.09375
- w_down: bfloat16 [28672, 4096], P('ep', 'tp'), may hold values from -0.125 to 0.125
Outputs:
- layer_out: bfloat16 [512, 4096], P(('groups', 'ep'), 'tp'), parts along dimension 0
The draws below stay inside these ranges and needn't reach their ends.
There are 2 independent parts, one for each index of `groups`. The reference program is written for one: setup_inputs(seed, part) draws one part's arguments, and reference() takes and returns one part's arrays. A program takes and returns all parts, laid end to end along the dimension named above; an argument that names none is the same for every part. Nothing has to cross between parts.
Inputs may be any that keep to these rules, and one draw needn't show every extreme that they name: `expert_ids`: each row names 2 different experts. In each aligned block of 64 rows (the rows of one index of ep) no expert is named by more than 36 rows, and in some blocks one expert is named by exactly 36 rows.
All inputs are finite; a program needn't handle non-finite values.
Results may differ from the reference program's by a relative error of at most 0.02.
Values may be sent and summed in bfloat16 or wider, within the bound.
A program may use at most 128 MiB of HBM per device.

```python
import math
import jax
import jax.numpy as jnp
import numpy as np
from jax import lax

D = 4096
EXPERTS = 4
TOP = 2
FF = 7168
TOK = 64
ATT = 4096
CAP = 36
TOKENS = 256
N_EP = 4
N_TP = 4


def draw_stream(key, part):
    key_base, key_rows = jax.random.split(jax.random.fold_in(key, 17))
    col_scale = jnp.exp(jnp.log(3.0) * jnp.arange(D, dtype=jnp.float32) / D) / jnp.sqrt(3.0)
    noise_base = jax.random.truncated_normal(key_base, -4.0, 4.0, (TOKENS, D), jnp.float32)
    row_scale = jnp.exp(jax.random.uniform(key_rows, (TOKENS, 1), jnp.float32, jnp.log(0.2), jnp.log(2.0)))
    return (noise_base * row_scale * col_scale[None, :]).astype(jnp.bfloat16)


def shard_levels(key, dims, cuts, low, high):
    loudness, own = 1.0, jax.random.fold_in(key, 6)
    for axis_at, blocks in cuts:
        heights = jnp.exp(jax.random.uniform(jax.random.fold_in(own, axis_at), (blocks,), jnp.float32, low / len(cuts), high / len(cuts)))
        loudness = loudness * jnp.repeat(heights, dims[axis_at] // blocks).reshape([-1 if axis == axis_at else 1 for axis in range(len(dims))])
    return loudness


def assign_block(key, own, number, rows, number_of, top, most, lean):
    sequence = jax.random.permutation(key, number_of)
    heavy_load, common = shares(number_of, rows * top, most, lean, True), shares(number_of, rows * top, most, lean, False)
    places = jnp.arange(number_of)

    def named(tallies, turn):
        used = int((tallies > 0).sum())
        fixed = max(1, used // 4)
        moved = fixed + (places - fixed + turn * (used - fixed)) % max(1, number_of - fixed)
        return jnp.zeros((number_of,), jnp.int32).at[sequence[jnp.where(places < fixed, places, moved)]].set(jnp.asarray(tallies, jnp.int32))

    tallies = jnp.where(number % 4 == 0, named(heavy_load, number // 4), named(common, number - number // 4 - 1))
    mixed = jax.random.permutation(jax.random.fold_in(own, 3), number_of)
    donor, receiver = mixed[0:number_of // 2 * 2:2], mixed[1:number_of // 2 * 2:2]
    room = jnp.minimum(tallies[donor] - 1, most - tallies[receiver]) // 2
    room = jnp.where((donor == sequence[0]) | (receiver == sequence[0]) | (tallies[receiver] == 0), 0, jnp.maximum(room, 0))
    moved = jax.random.randint(jax.random.fold_in(own, 4), (number_of // 2,), 0, 1 << 20) % (room + 1)
    tallies = tallies.at[donor].add(-moved).at[receiver].add(moved)
    members = jnp.searchsorted(jnp.cumsum(tallies), jnp.arange(rows * top), side="right").astype(jnp.int32)
    listing = members.reshape(top, rows).T
    listing = listing[jax.random.permutation(jax.random.fold_in(own, 1), rows)]
    turn = jax.random.randint(jax.random.fold_in(own, 2), (rows, 1), 0, top)
    return jnp.take_along_axis(listing, (jnp.arange(top)[None, :] + turn) % top, axis=1)


def shares(number_of, total, most, lean, full):
    loads = [(1 << 20) // math.isqrt(rank ** lean) + 1 for rank in range(1, number_of + 1)]
    largest = most if full else min(most, max(-(-total // number_of), total * loads[0] // sum(loads)))
    least = 1 if total - largest >= number_of - 1 else 0
    given, surplus = [largest] + [least] * (number_of - 1), total - largest - least * (number_of - 1)
    while surplus > 0:
        free = [i for i in range(1, number_of) if given[i] < largest] or [i for i in range(1, number_of) if given[i] < most]
        pool, remaining = sum([loads[i] for i in free]), surplus
        for i in free:
            extra = min(most - given[i], max(1, remaining * loads[i] // pool), surplus)
            given[i] = given[i] + extra
            surplus = surplus - extra
    return np.array(given)


def centred(rng, dims, deviation, limit, cuts=(), kind=jnp.bfloat16):
    level = shard_levels(rng, dims, cuts, -0.22, 0.18) if cuts else 1.0
    array = jax.random.normal(rng, dims, jnp.float32) * deviation * level
    return jnp.minimum(jnp.maximum(array, -limit), limit).astype(kind)


def setup_inputs(seed: int = 0, part: int = 0) -> dict:
    splits = jax.random.split(jax.random.key(seed), 10)
    part_keys = jax.random.split(jax.random.fold_in(splits[9], part), 10)
    context = centred(part_keys[0], (TOKENS, ATT), 1.0, 6.0, ((0, 4), (1, 4)))
    stream = draw_stream(jax.random.fold_in(jax.random.fold_in(splits[9], part), 71), part)
    out_proj = centred(splits[2], (ATT, D), ATT ** -0.5, 0.09375, ((0, 4), (1, 4)))
    norm_gain = jnp.clip(1.0 + 0.18 * jax.random.normal(splits[3], (D,), jnp.float32), 0.099609375, 1.8984375).astype(jnp.bfloat16)
    router = centred(splits[4], (D, EXPERTS), (2 * D) ** -0.5, 0.0625, ((0, 4),))
    expert_ids_keys = jax.random.split(jax.random.fold_in(part_keys[5], 1), TOKENS // TOK)
    expert_ids_turns = jax.random.permutation(jax.random.fold_in(part_keys[5], 3), TOKENS // TOK)
    expert_ids = jax.vmap(lambda own, number: assign_block(jax.random.fold_in(part_keys[5], 2), own, number, TOK, EXPERTS, TOP, CAP, 2))(expert_ids_keys, expert_ids_turns).reshape((TOKENS, TOP))
    w_gate = centred(splits[6], (D, EXPERTS * FF), D ** -0.5, 0.09375, ((0, 4), (1, 4)))
    w_up = centred(splits[7], (D, EXPERTS * FF), D ** -0.5, 0.09375, ((0, 4), (1, 4)))
    w_down = centred(splits[8], (EXPERTS * FF, D), (FF // 4) ** -0.5, 0.125, ((0, 4), (1, 4)))
    return {"context": context, "stream": stream, "out_proj": out_proj, "norm_gain": norm_gain, "router": router, "expert_ids": expert_ids, "w_gate": w_gate, "w_up": w_up, "w_down": w_down}


def rounded(tensor):
    return lax.optimization_barrier(tensor.astype(jnp.bfloat16)).astype(jnp.float32)

def reference(context, stream, out_proj, norm_gain, router, expert_ids, w_gate, w_up, w_down):
    head_cols = ATT // N_TP
    attention = jnp.zeros((TOKENS, D), jnp.float32)
    for device_lane in range(N_TP):
        low_index = device_lane * head_cols
        attention = attention + rounded(jnp.dot(context[:, low_index:low_index + head_cols], out_proj[low_index:low_index + head_cols], preferred_element_type=jnp.float32))
    hstate = (stream.astype(jnp.float32) + attention).astype(jnp.bfloat16)
    hfloat = hstate.astype(jnp.float32)
    inverse = lax.rsqrt(lax.optimization_barrier(jnp.mean(hfloat * hfloat, axis=1, keepdims=True)) + 1e-05)
    normed = hfloat * inverse * norm_gain.astype(jnp.float32)
    logits = jnp.dot(normed, router.astype(jnp.float32), precision=lax.Precision.HIGHEST)
    inputs = normed.astype(jnp.bfloat16)
    experts_range = jnp.arange(EXPERTS, dtype=jnp.int32)
    picked = expert_ids[:, :, None] == experts_range[None, None, :]
    chosen = lax.optimization_barrier(jnp.sum(jnp.where(picked, logits[:, None, :], jnp.zeros_like(logits[:, None, :])), axis=2))
    leading = jax.nn.sigmoid(chosen[:, 0] - chosen[:, 1])
    weights = jnp.stack([leading, 1.0 - leading], axis=1)
    flat_ids = expert_ids.reshape(N_EP, TOK * TOP)
    onehot = (flat_ids[:, :, None] == experts_range[None, None, :]).astype(jnp.int32)
    before = jnp.cumsum(onehot, axis=1) - onehot
    slot_index = lax.optimization_barrier(jnp.sum(before * onehot, axis=2))
    block_ids = jnp.arange(N_EP, dtype=jnp.int32)[:, None]
    target = ((flat_ids * N_EP + block_ids) * CAP + slot_index).reshape(TOKENS * TOP).astype(jnp.int32)
    owner_idx = (jnp.arange(TOKENS * TOP, dtype=jnp.int32) // TOP).astype(jnp.int32)
    slot_table = jnp.full((EXPERTS * N_EP * CAP,), TOKENS, jnp.int32).at[target].set(owner_idx)
    padded = jnp.concatenate([inputs, jnp.zeros((1, D), jnp.bfloat16)], axis=0)
    rows_all = padded[slot_table].reshape(EXPERTS, N_EP * CAP, D)
    part_rows = D // N_TP
    group_size = N_EP // EXPERTS
    block_size = FF // group_size
    outputs = []
    for expert in range(EXPERTS):
        chosen_rows = rows_all[expert]
        col_base = expert * FF
        gate_sum = jnp.zeros((N_EP * CAP, FF), jnp.float32)
        up_sum = jnp.zeros((N_EP * CAP, FF), jnp.float32)
        for device_lane in range(N_TP):
            low_index = device_lane * part_rows
            row_slice = chosen_rows[:, low_index:low_index + part_rows]
            gate_sum = gate_sum + rounded(jnp.dot(row_slice, w_gate[low_index:low_index + part_rows, col_base:col_base + FF], preferred_element_type=jnp.float32))
            up_sum = up_sum + rounded(jnp.dot(row_slice, w_up[low_index:low_index + part_rows, col_base:col_base + FF], preferred_element_type=jnp.float32))
        hidden = (jax.nn.silu(gate_sum) * up_sum).astype(jnp.bfloat16)
        expert_sum = jnp.zeros((N_EP * CAP, D), jnp.float32)
        for block_id in range(group_size):
            low_index = block_id * block_size
            expert_sum = expert_sum + rounded(jnp.dot(hidden[:, low_index:low_index + block_size], w_down[col_base + low_index:col_base + low_index + block_size], preferred_element_type=jnp.float32))
        outputs.append(expert_sum)
    expert_out = jnp.concatenate(outputs, axis=0)
    gathered = expert_out[target].reshape(TOKENS, TOP, D)
    expert_mix = lax.optimization_barrier(jnp.sum(gathered * weights[:, :, None], axis=1))
    return (hfloat + expert_mix).astype(jnp.bfloat16)
```

```python
import functools

import jax
import jax.numpy as jnp
from jax import lax
from jax.experimental import pallas as pl
from jax.experimental.pallas import tpu as pltpu
from jax.sharding import PartitionSpec as P

D = 4096
EXPERTS = 4
CAP = 36


def plain_device(context, stream, out_proj, norm_gain, router, expert_ids, w_gate, w_up, w_down):
    tok_rows = stream.shape[0]
    width_part = stream.shape[1]
    ep_count = lax.axis_size("ep")
    fanout = ep_count // EXPERTS
    columns = jnp.dot(
        lax.all_gather(context, "ep", axis=0, tiled=True),
        out_proj,
        preferred_element_type=jnp.float32,
    )
    head_part = lax.all_to_all(
        columns.astype(jnp.bfloat16), "ep", split_axis=0, concat_axis=1, tiled=True
    )
    attention = lax.psum_scatter(head_part, "tp", scatter_dimension=1, tiled=True).astype(
        jnp.float32
    )
    hstate = (stream.astype(jnp.float32) + attention).astype(jnp.bfloat16)
    hfloat = hstate.astype(jnp.float32)
    gain_vec = norm_gain.astype(jnp.float32)
    router_wide = router.astype(jnp.float32)
    squares = jnp.sum(hfloat * hfloat, axis=1)
    total_sq = lax.psum(squares, "tp")
    inverse = lax.rsqrt(total_sq / D + 1e-05)[:, None]
    normed = hfloat * inverse * gain_vec[None, :]
    logits = lax.psum(jnp.dot(normed, router_wide, precision=lax.Precision.HIGHEST), "tp")
    inputs = normed.astype(jnp.bfloat16)
    experts_range = jnp.arange(EXPERTS, dtype=jnp.int32)
    flat_ids = expert_ids.reshape(tok_rows * 2)
    onehot = (flat_ids[:, None] == experts_range[None, :]).astype(jnp.int32)
    before = jnp.cumsum(onehot, axis=0) - onehot
    slot_index = jnp.sum(before * onehot, axis=1)
    target = flat_ids * CAP + slot_index
    picked = onehot.reshape(tok_rows, 2, EXPERTS).astype(jnp.float32)
    chosen = jnp.sum(picked * logits[:, None, :], axis=2)
    leading = jax.nn.sigmoid(chosen[:, 0] - chosen[:, 1])
    weights = jnp.stack([leading, 1.0 - leading], axis=1)
    columns_all = jnp.arange(EXPERTS * CAP, dtype=jnp.int32)
    placement = (
        (target[:, None] == columns_all[None, :])
        .astype(jnp.float32)
        .reshape(tok_rows, 2, EXPERTS * CAP)
    )
    dispatch = jnp.sum(placement, axis=1)
    combine = jnp.sum(placement * weights[:, :, None], axis=1)
    sectioned = lax.dot_general(
        dispatch.astype(jnp.bfloat16),
        inputs,
        (((0,), (0,)), ((), ())),
        preferred_element_type=jnp.float32,
    ).astype(jnp.bfloat16)
    send_rows = jnp.broadcast_to(
        sectioned.reshape(EXPERTS, 1, CAP, width_part), (EXPERTS, fanout, CAP, width_part)
    ).reshape(ep_count, CAP, width_part)
    received = lax.all_to_all(send_rows, "ep", split_axis=0, concat_axis=0, tiled=True)
    slot_count = received.shape[1]
    flattened = received.reshape(ep_count * slot_count, width_part)
    gate_part = jnp.dot(flattened, w_gate, preferred_element_type=jnp.float32)
    up_part = jnp.dot(flattened, w_up, preferred_element_type=jnp.float32)
    gate_sum = lax.psum(gate_part.astype(jnp.bfloat16), "tp").astype(jnp.float32)
    up_sum = lax.psum(up_part.astype(jnp.bfloat16), "tp").astype(jnp.float32)
    hidden = (jax.nn.silu(gate_sum) * up_sum).astype(jnp.bfloat16)
    partial_value = jnp.dot(hidden, w_down, preferred_element_type=jnp.float32).astype(jnp.bfloat16)
    returned_rows = lax.all_to_all(
        partial_value.reshape(ep_count, slot_count, width_part),
        "ep",
        split_axis=0,
        concat_axis=0,
        tiled=True,
    )
    summed = jnp.sum(
        returned_rows.astype(jnp.float32).reshape(EXPERTS, fanout, CAP, width_part), axis=1
    ).reshape(EXPERTS * CAP, width_part)
    expert_mix = jnp.dot(combine, summed, precision=lax.Precision.HIGHEST)
    return (hfloat + expert_mix).astype(jnp.bfloat16)


MESH = pl.DeviceIdType.MESH
CHUNK = 256
WINDOW = 48
VMEM_BYTES = 67043328


def fused_kernel(
    n_ep,
    n_tp,
    pieces,
    ctx_ref,
    stream_ref,
    gain_ref,
    router_ref,
    ids_ref,
    proj_hbm,
    gate_hbm,
    up_hbm,
    down_hbm,
    out_ref,
    proj,
    gate,
    up,
    down,
    ctx_all,
    part,
    part_in,
    halves,
    landed,
    hkeep,
    x_all,
    rows,
    side,
    side_all,
    inv_all,
    slot_all,
    inv_rows,
    pair_out,
    pair_in,
    own_far,
    own_near,
    far_out,
    far_in,
    hid,
    acc,
    outb,
    ret,
    w_sem,
    ctx_send,
    ctx_recv,
    slot_send,
    slot_recv,
    part_send,
    part_recv,
    land_send,
    land_recv,
    side_send,
    side_recv,
    x_send,
    x_recv,
    inv_send,
    inv_recv,
    pair_send,
    pair_recv,
    far_send,
    far_recv,
    hx_send,
    hx_recv,
    hc_send,
    hc_recv,
    hf_send,
    hf_recv,
    ret_send,
    ret_recv,
):
    me = lax.axis_index("ep")
    lane = lax.axis_index("tp")
    core = lax.rem(lane, 2)
    side_x = lane // 2
    mate = 2 * side_x + (1 - core)
    across = 2 * (1 - side_x) + core
    tok, width = stream_ref.shape
    depth = n_tp * width
    quarter = gate.shape[1] // n_tp
    count = quarter // CHUNK
    slots = rows.shape[0]
    f32, bf16 = jnp.float32, jnp.bfloat16

    loads = {}
    number = 0
    for name, src, dst in (("p", proj_hbm, proj), ("g", gate_hbm, gate), ("u", up_hbm, up), ("d", down_hbm, down)):
        step = src.shape[0] // pieces
        group = []
        for p in range(pieces):
            copy = pltpu.make_async_copy(
                src.at[pl.ds(p * step, step)], dst.at[pl.ds(p * step, step)], w_sem.at[number]
            )
            copy.start()
            group.append(copy)
            number += 1
        loads[name] = group

    barrier = pltpu.get_barrier_semaphore()
    for de in range(n_ep):
        for dt in range(n_tp):
            if de or dt:
                pl.semaphore_signal(
                    barrier,
                    inc=1,
                    device_id={"ep": lax.rem(me + de, n_ep), "tp": lax.rem(lane + dt, n_tp)},
                    device_id_type=MESH,
                )

    ids = ids_ref[...]
    lanes = lax.broadcasted_iota(jnp.int32, (tok, 128), 1)
    named = jnp.where((ids[:, 0:1] == lanes) | (ids[:, 1:2] == lanes), 1.0, 0.0).astype(f32)
    row_i = lax.broadcasted_iota(jnp.int32, (tok, tok), 0)
    col_i = lax.broadcasted_iota(jnp.int32, (tok, tok), 1)
    lower = jnp.where(col_i < row_i, 1.0, 0.0).astype(bf16)
    rank = jnp.dot(lower, named.astype(bf16), preferred_element_type=f32)
    slot_local = jnp.where(named > 0.5, rank, -4096.0)
    slot_all[me] = slot_local

    pl.semaphore_wait(barrier, n_ep * n_tp - 1)

    def over_ep(src, dst, sends, recvs):
        copies = []
        for k in range(1, n_ep):
            copy = pltpu.make_async_remote_copy(
                src_ref=src,
                dst_ref=dst,
                send_sem=sends.at[k - 1],
                recv_sem=recvs.at[k - 1],
                device_id={"ep": lax.rem(me + k, n_ep)},
                device_id_type=MESH,
            )
            copy.start()
            copies.append(copy)
        return copies

    ctx_copies = over_ep(ctx_ref, ctx_all.at[me], ctx_send, ctx_recv)
    slot_copies = over_ep(slot_all.at[me], slot_all.at[me], slot_send, slot_recv)

    for copy in loads["p"]:
        copy.wait()
    for k in range(n_ep):
        block = lax.rem(me + n_ep - k, n_ep)
        if k:
            ctx_copies[k - 1].wait_recv()
            value = ctx_all[block]
        else:
            value = ctx_ref[...]
        part[block] = jnp.dot(value, proj[...], preferred_element_type=f32).astype(bf16)

    part_copies = []
    for i in range(2):
        block = (1 - core) + 2 * i
        copy = pltpu.make_async_remote_copy(
            src_ref=part.at[block],
            dst_ref=part_in.at[i],
            send_sem=part_send.at[i],
            recv_sem=part_recv.at[i],
            device_id={"tp": mate},
            device_id_type=MESH,
        )
        copy.start()
        part_copies.append(copy)
    land_copies = []
    for i in range(2):
        block = core + 2 * i
        part_copies[i].wait_recv()
        halves[i] = (part[block].astype(f32) + part_in[i].astype(f32)).astype(bf16)
        copy = pltpu.make_async_remote_copy(
            src_ref=halves.at[i],
            dst_ref=landed.at[side_x],
            send_sem=land_send.at[i],
            recv_sem=land_recv.at[side_x],
            device_id={"ep": block, "tp": me},
            device_id_type=MESH,
        )
        here = jnp.logical_and(block == me, me == lane)

        @pl.when(here)
        def _():
            landed[side_x] = halves[i]

        @pl.when(jnp.logical_not(here))
        def _():
            copy.start()

        land_copies.append((copy, here))

    for j in range(2):
        source = 2 * j + lax.rem(me, 2)
        mine = jnp.logical_and(me == lane, source == lane)

        @pl.when(jnp.logical_not(mine))
        def _():
            pltpu.make_async_remote_copy(
                src_ref=halves.at[0],
                dst_ref=landed.at[j],
                send_sem=land_send.at[0],
                recv_sem=land_recv.at[j],
                device_id={"tp": mate},
                device_id_type=MESH,
            ).wait_recv()

    attention = landed[0].astype(f32) + landed[1].astype(f32)
    hstate = (stream_ref[...].astype(f32) + attention).astype(bf16)
    hkeep[...] = hstate
    hfloat = hstate.astype(f32)
    scaled = hfloat * gain_ref[...].astype(f32)
    x_all[me] = scaled.astype(bf16)
    x_copies = over_ep(x_all.at[me], x_all.at[me], x_send, x_recv)

    side[...] = jnp.zeros_like(side)
    side[:, 0:EXPERTS] = jnp.dot(
        scaled, router_ref[...].astype(f32), precision=lax.Precision.HIGHEST, preferred_element_type=f32
    )
    side[:, EXPERTS : EXPERTS + 1] = jnp.sum(hfloat * hfloat, axis=1, keepdims=True)
    side_copies = []
    for k in range(1, n_tp):
        copy = pltpu.make_async_remote_copy(
            src_ref=side,
            dst_ref=side_all.at[k - 1],
            send_sem=side_send.at[k - 1],
            recv_sem=side_recv.at[k - 1],
            device_id={"tp": lax.rem(lane + k, n_tp)},
            device_id_type=MESH,
        )
        copy.start()
        side_copies.append(copy)
    total = side[...]
    for k in range(1, n_tp):
        side_copies[k - 1].wait_recv()
        total = total + side_all[k - 1]
    inverse = lax.rsqrt(total[:, EXPERTS : EXPERTS + 1] / depth + 1e-05)
    logits = total * inverse
    first = jnp.sum(jnp.where(ids[:, 0:1] == lanes, logits, 0.0), axis=1, keepdims=True)
    second = jnp.sum(jnp.where(ids[:, 1:2] == lanes, logits, 0.0), axis=1, keepdims=True)
    leading = jax.nn.sigmoid(first - second)
    inv_all[me] = jnp.broadcast_to(inverse, (tok, 128))
    inv_copies = over_ep(inv_all.at[me], inv_all.at[me], inv_send, inv_recv)

    for copy in slot_copies:
        copy.wait_recv()
    columns = []
    wide = lax.broadcasted_iota(jnp.int32, (tok, 256), 1).astype(f32)
    for b in range(n_ep):
        picked = jnp.sum(jnp.where(lanes == me, slot_all[b], 0.0), axis=1, keepdims=True)
        columns.append(jnp.where(picked + float(b * CAP) == wide, 1.0, 0.0).astype(f32))
    chooser = jnp.transpose(jnp.concatenate(columns, axis=0))[:slots]
    for copy in x_copies:
        copy.wait_recv()
    rows[...] = jnp.dot(
        chooser.astype(bf16), x_all[...].reshape(n_ep * tok, width), preferred_element_type=f32
    ).astype(bf16)
    for copy in inv_copies:
        copy.wait_recv()
    inv_rows[...] = jnp.dot(
        chooser,
        inv_all[...].reshape(n_ep * tok, 128),
        precision=lax.Precision.HIGHEST,
        preferred_element_type=f32,
    )
    acc[...] = jnp.zeros_like(acc)
    for name in ("g", "u", "d"):
        for copy in loads[name]:
            copy.wait()

    def pair_copy(i):
        return pltpu.make_async_remote_copy(
            src_ref=pair_out.at[i], dst_ref=pair_in.at[i], send_sem=pair_send.at[i], recv_sem=pair_recv.at[i],
            device_id={"tp": mate}, device_id_type=MESH,
        )

    def far_copy(i):
        return pltpu.make_async_remote_copy(
            src_ref=far_out.at[i], dst_ref=far_in.at[i], send_sem=far_send.at[i], recv_sem=far_recv.at[i],
            device_id={"tp": across}, device_id_type=MESH,
        )

    own_q = 2 * core + side_x
    far_q = 2 * core + (1 - side_x)

    def hid_copy(i, q, target, sends, recvs):
        return pltpu.make_async_remote_copy(
            src_ref=hid.at[q, i], dst_ref=hid.at[q, i], send_sem=sends.at[i], recv_sem=recvs.at[i],
            device_id={"tp": target}, device_id_type=MESH,
        )

    def columns_of(weight, q, i):
        return weight[:, pl.ds(pl.multiple_of(q * quarter + i * CHUNK, CHUNK), CHUNK)]

    def step(s, carry):
        @pl.when(s < count)
        def _():
            i = s
            value = rows[...]
            for j in range(2):
                for m, weight in enumerate((gate, up)):
                    pair_out[i, 2 * j + m] = jnp.dot(
                        value, columns_of(weight, 2 * (1 - core) + j, i), preferred_element_type=f32
                    ).astype(bf16)
            pair_copy(i).start()
            for m, weight in enumerate((gate, up)):
                own_far[lax.rem(i, 2), m] = jnp.dot(
                    value, columns_of(weight, far_q, i), preferred_element_type=f32
                )
                own_near[i, m] = jnp.dot(
                    value, columns_of(weight, own_q, i), preferred_element_type=f32
                )

        @pl.when(jnp.logical_and(s >= 1, s < count + 1))
        def _():
            i = s - 1
            pair_copy(i).wait_recv()
            for m in range(2):
                far_out[i, m] = (
                    own_far[lax.rem(i, 2), m] + pair_in[i, 2 * (1 - side_x) + m].astype(f32)
                ).astype(bf16)
            far_copy(i).start()
            for m in range(2):
                own_near[i, m] = own_near[i, m] + pair_in[i, 2 * side_x + m].astype(f32)

        @pl.when(jnp.logical_and(s >= 3, s < count + 3))
        def _():
            i = s - 3
            far_copy(i).wait_recv()
            scale = inv_rows[:, 0:1]
            g = (own_near[i, 0] + far_in[i, 0].astype(f32)) * scale
            u = (own_near[i, 1] + far_in[i, 1].astype(f32)) * scale
            hid[own_q, i] = (g / (1.0 + jnp.exp(-g)) * u).astype(bf16)
            hid_copy(i, own_q, across, hx_send, hx_recv).start()
            hid_copy(i, own_q, mate, hc_send, hc_recv).start()

        @pl.when(jnp.logical_and(s >= 4, s < count + 4))
        def _():
            i = s - 4
            hid_copy(i, far_q, across, hx_send, hx_recv).wait_recv()
            hid_copy(i, far_q, mate, hf_send, hf_recv).start()

        @pl.when(s >= 5)
        def _():
            i = s - 5
            hid_copy(i, own_q, mate, hc_send, hc_recv).wait_recv()
            hid_copy(i, far_q, mate, hf_send, hf_recv).wait_recv()
            value = acc[...]
            for q in range(4):
                value = value + jnp.dot(
                    hid[q, i],
                    down[pl.ds(pl.multiple_of(q * quarter + i * CHUNK, CHUNK), CHUNK), :],
                    preferred_element_type=f32,
                )
            acc[...] = value

        return carry

    lax.fori_loop(0, count + 5, step, 0)

    outb[...] = acc[...].astype(bf16)
    ret_copies = []
    for k in range(1, n_ep):
        peer = lax.rem(me + k, n_ep)
        copy = pltpu.make_async_remote_copy(
            src_ref=outb.at[pl.ds(pl.multiple_of(peer * (CAP // 16 * 16), 16), WINDOW)],
            dst_ref=ret.at[me],
            send_sem=ret_send.at[k - 1],
            recv_sem=ret_recv.at[k - 1],
            device_id={"ep": peer},
            device_id_type=MESH,
        )
        copy.start()
        ret_copies.append(copy)
    ret[me] = outb[pl.ds(pl.multiple_of(me * (CAP // 16 * 16), 16), WINDOW), :]
    shift = (me * (CAP - CAP // 16 * 16)).astype(f32)
    window = lax.broadcasted_iota(jnp.int32, (tok, WINDOW), 1).astype(f32)

    def returned(source):
        at_source = lanes == source
        place = jnp.sum(jnp.where(at_source, slot_all[me], 0.0), axis=1, keepdims=True) + shift
        chosen = jnp.where(place == window, 1.0, 0.0).astype(bf16)
        weight = jnp.where(
            ids[:, 0:1] == source, leading, jnp.where(ids[:, 1:2] == source, 1.0 - leading, 0.0)
        )
        return weight * jnp.dot(chosen, ret[source], preferred_element_type=f32)

    mixed = hkeep[...].astype(f32) + returned(me)
    for k in range(1, n_ep):
        ret_copies[k - 1].wait_recv()
        mixed = mixed + returned(lax.rem(me + n_ep - k, n_ep))
    out_ref[...] = mixed.astype(bf16)

    for copy in ctx_copies + slot_copies + part_copies + side_copies + x_copies + inv_copies + ret_copies:
        copy.wait_send()
    for copy, here in land_copies:

        @pl.when(jnp.logical_not(here))
        def _():
            copy.wait_send()

    def drain(i, carry):
        pair_copy(i).wait_send()
        far_copy(i).wait_send()
        hid_copy(i, own_q, across, hx_send, hx_recv).wait_send()
        hid_copy(i, own_q, mate, hc_send, hc_recv).wait_send()
        hid_copy(i, far_q, mate, hf_send, hf_recv).wait_send()
        return carry

    lax.fori_loop(0, count, drain, 0)


def fused_device(context, stream, out_proj, norm_gain, router, expert_ids, w_gate, w_up, w_down):
    n_ep, n_tp = lax.axis_size("ep"), lax.axis_size("tp")
    tok, width = stream.shape
    heads = context.shape[1]
    hidden = w_gate.shape[1]
    cols = out_proj.shape[1]
    slots = n_ep * CAP
    count = hidden // n_tp // CHUNK
    pieces = 4
    bf16, f32 = jnp.bfloat16, jnp.float32
    vmem, hbm = pl.BlockSpec(memory_space=pltpu.VMEM), pl.BlockSpec(memory_space=pl.ANY)
    dma = lambda n: pltpu.SemaphoreType.DMA((n,))
    scratch = [
        pltpu.VMEM(out_proj.shape, bf16),
        pltpu.VMEM(w_gate.shape, bf16),
        pltpu.VMEM(w_up.shape, bf16),
        pltpu.VMEM(w_down.shape, bf16),
        pltpu.VMEM((n_ep, tok, heads), bf16),
        pltpu.VMEM((n_ep, tok, cols), bf16),
        pltpu.VMEM((2, tok, cols), bf16),
        pltpu.VMEM((2, tok, cols), bf16),
        pltpu.VMEM((2, tok, cols), bf16),
        pltpu.VMEM((tok, width), bf16),
        pltpu.VMEM((n_ep, tok, width), bf16),
        pltpu.VMEM((slots, width), bf16),
        pltpu.VMEM((tok, 128), f32),
        pltpu.VMEM((n_tp - 1, tok, 128), f32),
        pltpu.VMEM((n_ep, tok, 128), f32),
        pltpu.VMEM((n_ep, tok, 128), f32),
        pltpu.VMEM((slots, 128), f32),
        pltpu.VMEM((count, 4, slots, CHUNK), bf16),
        pltpu.VMEM((count, 4, slots, CHUNK), bf16),
        pltpu.VMEM((2, 2, slots, CHUNK), f32),
        pltpu.VMEM((count, 2, slots, CHUNK), f32),
        pltpu.VMEM((count, 2, slots, CHUNK), bf16),
        pltpu.VMEM((count, 2, slots, CHUNK), bf16),
        pltpu.VMEM((4, count, slots, CHUNK), bf16),
        pltpu.VMEM((slots, width), f32),
        pltpu.VMEM((slots, width), bf16),
        pltpu.VMEM((n_ep, WINDOW, width), bf16),
        dma(4 * pieces),
    ]
    for size in (n_ep - 1, n_ep - 1, 2, 2, n_tp - 1, n_ep - 1, n_ep - 1, count, count, count, count, count, n_ep - 1):
        scratch += [dma(size), dma(size)]
    return pl.pallas_call(
        functools.partial(fused_kernel, n_ep, n_tp, pieces),
        out_shape=jax.ShapeDtypeStruct((tok, width), bf16),
        in_specs=[vmem] * 5 + [hbm] * 4,
        out_specs=vmem,
        scratch_shapes=scratch,
        compiler_params=pltpu.CompilerParams(
            collective_id=0, has_side_effects=True, vmem_limit_bytes=VMEM_BYTES
        ),
        name="fused_layer",
    )(context, stream, norm_gain.reshape(1, width), router, expert_ids, out_proj, w_gate, w_up, w_down)


def solution(mesh):
    sizes = dict(mesh.shape)
    fused = sizes["tp"] == 4 and sizes["ep"] == EXPERTS
    return jax.shard_map(
        fused_device if fused else plain_device,
        mesh=mesh,
        in_specs=(
            P(("groups", "ep"), "tp"),
            P(("groups", "ep"), "tp"),
            P("tp", "ep"),
            P("tp"),
            P("tp", None),
            P(("groups", "ep"), None),
            P("tp", "ep"),
            P("tp", "ep"),
            P("ep", "tp"),
        ),
        out_specs=P(("groups", "ep"), "tp"),
        check_vma=False,
    )
```

```python
import functools

import jax
import jax.numpy as jnp
from jax import lax
from jax.experimental import pallas as pl
from jax.experimental.pallas import tpu as pltpu
from jax.sharding import PartitionSpec as P

D = 4096
EXPERTS = 4
CAP = 36


def plain_device(context, stream, out_proj, norm_gain, router, expert_ids, w_gate, w_up, w_down):
    tok_rows = stream.shape[0]
    width_part = stream.shape[1]
    ep_count = lax.axis_size("ep")
    fanout = ep_count // EXPERTS
    columns = jnp.dot(
        lax.all_gather(context, "ep", axis=0, tiled=True),
        out_proj,
        preferred_element_type=jnp.float32,
    )
    head_part = lax.all_to_all(
        columns.astype(jnp.bfloat16), "ep", split_axis=0, concat_axis=1, tiled=True
    )
    attention = lax.psum_scatter(head_part, "tp", scatter_dimension=1, tiled=True).astype(
        jnp.float32
    )
    hstate = (stream.astype(jnp.float32) + attention).astype(jnp.bfloat16)
    hfloat = hstate.astype(jnp.float32)
    gain_vec = norm_gain.astype(jnp.float32)
    router_wide = router.astype(jnp.float32)
    squares = jnp.sum(hfloat * hfloat, axis=1)
    total_sq = lax.psum(squares, "tp")
    inverse = lax.rsqrt(total_sq / D + 1e-05)[:, None]
    normed = hfloat * inverse * gain_vec[None, :]
    logits = lax.psum(jnp.dot(normed, router_wide, precision=lax.Precision.HIGHEST), "tp")
    inputs = normed.astype(jnp.bfloat16)
    experts_range = jnp.arange(EXPERTS, dtype=jnp.int32)
    flat_ids = expert_ids.reshape(tok_rows * 2)
    onehot = (flat_ids[:, None] == experts_range[None, :]).astype(jnp.int32)
    before = jnp.cumsum(onehot, axis=0) - onehot
    slot_index = jnp.sum(before * onehot, axis=1)
    target = flat_ids * CAP + slot_index
    picked = onehot.reshape(tok_rows, 2, EXPERTS).astype(jnp.float32)
    chosen = jnp.sum(picked * logits[:, None, :], axis=2)
    leading = jax.nn.sigmoid(chosen[:, 0] - chosen[:, 1])
    weights = jnp.stack([leading, 1.0 - leading], axis=1)
    columns_all = jnp.arange(EXPERTS * CAP, dtype=jnp.int32)
    placement = (
        (target[:, None] == columns_all[None, :])
        .astype(jnp.float32)
        .reshape(tok_rows, 2, EXPERTS * CAP)
    )
    dispatch = jnp.sum(placement, axis=1)
    combine = jnp.sum(placement * weights[:, :, None], axis=1)
    sectioned = lax.dot_general(
        dispatch.astype(jnp.bfloat16),
        inputs,
        (((0,), (0,)), ((), ())),
        preferred_element_type=jnp.float32,
    ).astype(jnp.bfloat16)
    send_rows = jnp.broadcast_to(
        sectioned.reshape(EXPERTS, 1, CAP, width_part), (EXPERTS, fanout, CAP, width_part)
    ).reshape(ep_count, CAP, width_part)
    received = lax.all_to_all(send_rows, "ep", split_axis=0, concat_axis=0, tiled=True)
    slot_count = received.shape[1]
    flattened = received.reshape(ep_count * slot_count, width_part)
    gate_part = jnp.dot(flattened, w_gate, preferred_element_type=jnp.float32)
    up_part = jnp.dot(flattened, w_up, preferred_element_type=jnp.float32)
    gate_sum = lax.psum(gate_part.astype(jnp.bfloat16), "tp").astype(jnp.float32)
    up_sum = lax.psum(up_part.astype(jnp.bfloat16), "tp").astype(jnp.float32)
    hidden = (jax.nn.silu(gate_sum) * up_sum).astype(jnp.bfloat16)
    partial_value = jnp.dot(hidden, w_down, preferred_element_type=jnp.float32).astype(jnp.bfloat16)
    returned_rows = lax.all_to_all(
        partial_value.reshape(ep_count, slot_count, width_part),
        "ep",
        split_axis=0,
        concat_axis=0,
        tiled=True,
    )
    summed = jnp.sum(
        returned_rows.astype(jnp.float32).reshape(EXPERTS, fanout, CAP, width_part), axis=1
    ).reshape(EXPERTS * CAP, width_part)
    expert_mix = jnp.dot(combine, summed, precision=lax.Precision.HIGHEST)
    return (hfloat + expert_mix).astype(jnp.bfloat16)


MESH = pl.DeviceIdType.MESH
CHUNK = 256
LAG_SUM, LAG_PASS, LAG_DOWN = 4, 7, 9
WINDOW = 40
ALIGN = 8
VMEM_BYTES = 67043328


def fused_kernel(
    n_ep,
    n_tp,
    pieces,
    ctx_ref,
    stream_ref,
    gain_ref,
    router_ref,
    ids_ref,
    proj_hbm,
    gate_hbm,
    up_hbm,
    down_hbm,
    out_ref,
    proj,
    gate,
    up,
    down,
    ctx_all,
    part,
    part_in,
    halves,
    landed,
    hkeep,
    x_all,
    rows,
    side,
    side_all,
    inv_all,
    slot_all,
    inv_rows,
    chooser,
    mix,
    pair_out,
    pair_in,
    own_far,
    own_near,
    far_out,
    far_in,
    hid,
    acc,
    outb,
    ret,
    w_sem,
    ctx_send,
    ctx_recv,
    slot_send,
    slot_recv,
    part_send,
    part_recv,
    land_send,
    land_recv,
    side_send,
    side_recv,
    x_send,
    x_recv,
    inv_send,
    inv_recv,
    pair_send,
    pair_recv,
    far_send,
    far_recv,
    hx_send,
    hx_recv,
    hc_send,
    hc_recv,
    hf_send,
    hf_recv,
    ret_send,
    ret_recv,
):
    me = lax.axis_index("ep")
    lane = lax.axis_index("tp")
    core = lax.rem(lane, 2)
    side_x = lane // 2
    mate = 2 * side_x + (1 - core)
    across = 2 * (1 - side_x) + core
    tok, width = stream_ref.shape
    depth = n_tp * width
    quarter = gate.shape[1] // n_tp
    count = quarter // CHUNK
    total_steps = 2 * count
    slots = rows.shape[1]
    f32, bf16 = jnp.float32, jnp.bfloat16
    peers = (me, me + 1 - 2 * lax.rem(me, 2), lax.rem(me + 2, 4), 3 - me)

    loads = {}
    number = 0
    for name, src, dst in (("p", proj_hbm, proj), ("g", gate_hbm, gate), ("u", up_hbm, up), ("d", down_hbm, down)):
        step = src.shape[0] // pieces
        group = []
        for p in range(pieces):
            copy = pltpu.make_async_copy(
                src.at[pl.ds(p * step, step)], dst.at[pl.ds(p * step, step)], w_sem.at[number]
            )
            copy.start()
            group.append(copy)
            number += 1
        loads[name] = group

    barrier = pltpu.get_barrier_semaphore()
    for de in range(n_ep):
        for dt in range(n_tp):
            if de or dt:
                pl.semaphore_signal(
                    barrier,
                    inc=1,
                    device_id={"ep": lax.rem(me + de, n_ep), "tp": lax.rem(lane + dt, n_tp)},
                    device_id_type=MESH,
                )

    experts = lax.broadcasted_iota(jnp.int32, (128, tok), 0)
    is_first = jnp.transpose(jnp.where(ids_ref[0:1, :] == experts, 1.0, 0.0).astype(f32))
    is_second = jnp.transpose(jnp.where(ids_ref[1:2, :] == experts, 1.0, 0.0).astype(f32))
    named = is_first + is_second
    lanes = lax.broadcasted_iota(jnp.int32, (tok, 128), 1)
    row_i = lax.broadcasted_iota(jnp.int32, (tok, tok), 0)
    col_i = lax.broadcasted_iota(jnp.int32, (tok, tok), 1)
    lower = jnp.where(col_i < row_i, 1.0, 0.0).astype(bf16)
    rank = jnp.dot(lower, named.astype(bf16), preferred_element_type=f32)
    slot_all[0] = jnp.where(named > 0.5, rank, -4096.0)

    pl.semaphore_wait(barrier, n_ep * n_tp - 1)

    def over_ep(src, dst, sends, recvs):
        copies = []
        for k in range(1, n_ep):
            copy = pltpu.make_async_remote_copy(
                src_ref=src,
                dst_ref=dst.at[k],
                send_sem=sends.at[k - 1],
                recv_sem=recvs.at[k - 1],
                device_id={"ep": peers[k]},
                device_id_type=MESH,
            )
            copy.start()
            copies.append(copy)
        return copies

    ctx_copies = over_ep(ctx_ref, ctx_all, ctx_send, ctx_recv)
    slot_copies = over_ep(slot_all.at[0], slot_all, slot_send, slot_recv)

    for copy in loads["p"]:
        copy.wait()
    part_copies, land_copies = [], []
    for i in range(2):
        pair = me // 2 if i == 0 else 1 - me // 2
        for k in (2 * i, 2 * i + 1):
            if k:
                ctx_copies[k - 1].wait_recv()
                value = ctx_all[k]
            else:
                value = ctx_ref[...]
            part[peers[k]] = jnp.dot(value, proj[...], preferred_element_type=f32).astype(bf16)
        copy = pltpu.make_async_remote_copy(
            src_ref=part.at[2 * pair + (1 - core)],
            dst_ref=part_in.at[i],
            send_sem=part_send.at[i],
            recv_sem=part_recv.at[i],
            device_id={"tp": mate},
            device_id_type=MESH,
        )
        copy.start()
        part_copies.append(copy)
        block = 2 * pair + core
        copy.wait_recv()
        halves[i] = (part[block].astype(f32) + part_in[i].astype(f32)).astype(bf16)
        copy = pltpu.make_async_remote_copy(
            src_ref=halves.at[i],
            dst_ref=landed.at[side_x],
            send_sem=land_send.at[i],
            recv_sem=land_recv.at[side_x],
            device_id={"ep": block, "tp": me},
            device_id_type=MESH,
        )
        here = jnp.logical_and(block == me, me == lane)

        @pl.when(here)
        def _():
            landed[side_x] = halves[i]

        @pl.when(jnp.logical_not(here))
        def _():
            copy.start()

        land_copies.append((copy, here))

    for j in range(2):
        source = 2 * j + lax.rem(me, 2)
        mine = jnp.logical_and(me == lane, source == lane)

        @pl.when(jnp.logical_not(mine))
        def _():
            pltpu.make_async_remote_copy(
                src_ref=halves.at[0],
                dst_ref=landed.at[j],
                send_sem=land_send.at[0],
                recv_sem=land_recv.at[j],
                device_id={"tp": mate},
                device_id_type=MESH,
            ).wait_recv()

    attention = landed[0].astype(f32) + landed[1].astype(f32)
    hstate = (stream_ref[...].astype(f32) + attention).astype(bf16)
    hkeep[...] = hstate
    hfloat = hstate.astype(f32)
    scaled = hfloat * gain_ref[...].astype(f32).reshape(1, width)
    x_all[0] = scaled.astype(bf16)
    x_copies = over_ep(x_all.at[0], x_all, x_send, x_recv)

    side[...] = jnp.zeros_like(side)
    side[:, 0:EXPERTS] = lax.dot_general(
        scaled,
        router_ref[...].astype(f32),
        (((1,), (1,)), ((), ())),
        precision=lax.Precision.HIGHEST,
        preferred_element_type=f32,
    )
    side[:, EXPERTS : EXPERTS + 1] = jnp.sum(hfloat * hfloat, axis=1, keepdims=True)
    side_copies = []
    for k in range(1, n_tp):
        copy = pltpu.make_async_remote_copy(
            src_ref=side,
            dst_ref=side_all.at[k - 1],
            send_sem=side_send.at[k - 1],
            recv_sem=side_recv.at[k - 1],
            device_id={"tp": lax.rem(lane + k, n_tp)},
            device_id_type=MESH,
        )
        copy.start()
        side_copies.append(copy)
    total = side[...]
    for k in range(1, n_tp):
        side_copies[k - 1].wait_recv()
        total = total + side_all[k - 1]
    inverse = lax.rsqrt(total[:, EXPERTS : EXPERTS + 1] / depth + 1e-05)
    logits = total * inverse
    first = jnp.sum(is_first * logits, axis=1, keepdims=True)
    second = jnp.sum(is_second * logits, axis=1, keepdims=True)
    leading = jax.nn.sigmoid(first - second)
    mix[...] = is_first * leading + is_second * (1.0 - leading)
    inv_all[0] = jnp.broadcast_to(inverse, (tok, 128))
    inv_copies = over_ep(inv_all.at[0], inv_all, inv_send, inv_recv)

    for copy in slot_copies:
        copy.wait_recv()
    wide = lanes.astype(f32)
    for g in range(2):
        columns = []
        for p in range(2):
            picked = jnp.sum(jnp.where(lanes == me, slot_all[2 * g + p], 0.0), axis=1, keepdims=True)
            columns.append(jnp.where(picked + float(p * CAP) == wide, 1.0, 0.0).astype(f32))
        chooser[g] = jnp.transpose(jnp.concatenate(columns, axis=0))[:slots]

    def fill_rows(g):
        rows[g] = jnp.dot(
            chooser[g].astype(bf16),
            x_all[2 * g : 2 * g + 2].reshape(2 * tok, width),
            preferred_element_type=f32,
        ).astype(bf16)

    def fill_inverse(g):
        inv_rows[g] = jnp.dot(
            chooser[g],
            inv_all[2 * g : 2 * g + 2].reshape(2 * tok, 128),
            precision=lax.Precision.HIGHEST,
            preferred_element_type=f32,
        )

    acc[...] = jnp.zeros_like(acc)
    for name in ("g", "u", "d"):
        for copy in loads[name]:
            copy.wait()
    x_copies[0].wait_recv()
    fill_rows(0)

    def ret_copy(k):
        return pltpu.make_async_remote_copy(
            src_ref=outb.at[k // 2, pl.ds((k % 2) * (CAP // ALIGN * ALIGN), WINDOW)],
            dst_ref=ret.at[k],
            send_sem=ret_send.at[k - 1],
            recv_sem=ret_recv.at[k - 1],
            device_id={"ep": peers[k]},
            device_id_type=MESH,
        )

    def pair_copy(i):
        return pltpu.make_async_remote_copy(
            src_ref=pair_out.at[i], dst_ref=pair_in.at[i], send_sem=pair_send.at[i], recv_sem=pair_recv.at[i],
            device_id={"tp": mate}, device_id_type=MESH,
        )

    def far_copy(i):
        return pltpu.make_async_remote_copy(
            src_ref=far_out.at[i], dst_ref=far_in.at[i], send_sem=far_send.at[i], recv_sem=far_recv.at[i],
            device_id={"tp": across}, device_id_type=MESH,
        )

    own_q = 2 * core + side_x
    far_q = 2 * core + (1 - side_x)

    def hid_copy(i, q, target, sends, recvs):
        return pltpu.make_async_remote_copy(
            src_ref=hid.at[q, i], dst_ref=hid.at[q, i], send_sem=sends.at[i], recv_sem=recvs.at[i],
            device_id={"tp": target}, device_id_type=MESH,
        )

    def columns_of(weight, q, i):
        return weight[:, pl.ds(pl.multiple_of(q * quarter + lax.rem(i, count) * CHUNK, CHUNK), CHUNK)]

    def step(s, carry):
        @pl.when(s == count)
        def _():
            for k in (2, 3):
                x_copies[k - 1].wait_recv()
            fill_rows(1)

        @pl.when(s < total_steps)
        def _():
            i = s
            value = rows[i // count]
            for j in range(2):
                for m, weight in enumerate((gate, up)):
                    pair_out[i, 2 * j + m] = jnp.dot(
                        value, columns_of(weight, 2 * (1 - core) + j, i), preferred_element_type=f32
                    ).astype(bf16)
            pair_copy(i).start()
            for m, weight in enumerate((gate, up)):
                own_far[lax.rem(i, 2), m] = jnp.dot(
                    value, columns_of(weight, far_q, i), preferred_element_type=f32
                )
                own_near[i, m] = jnp.dot(
                    value, columns_of(weight, own_q, i), preferred_element_type=f32
                )

        @pl.when(jnp.logical_and(s >= 1, s < total_steps + 1))
        def _():
            i = s - 1
            pair_copy(i).wait_recv()
            for m in range(2):
                far_out[i, m] = (
                    own_far[lax.rem(i, 2), m] + pair_in[i, 2 * (1 - side_x) + m].astype(f32)
                ).astype(bf16)
            far_copy(i).start()
            for m in range(2):
                own_near[i, m] = own_near[i, m] + pair_in[i, 2 * side_x + m].astype(f32)

        @pl.when(s == LAG_SUM)
        def _():
            inv_copies[0].wait_recv()
            fill_inverse(0)

        @pl.when(s == count + LAG_SUM)
        def _():
            for k in (2, 3):
                inv_copies[k - 1].wait_recv()
            fill_inverse(1)

        @pl.when(jnp.logical_and(s >= LAG_SUM, s < total_steps + LAG_SUM))
        def _():
            i = s - LAG_SUM
            far_copy(i).wait_recv()
            scale = inv_rows[i // count, :, 0:1]
            g = (own_near[i, 0] + far_in[i, 0].astype(f32)) * scale
            u = (own_near[i, 1] + far_in[i, 1].astype(f32)) * scale
            hid[own_q, i] = (g / (1.0 + jnp.exp(-g)) * u).astype(bf16)
            hid_copy(i, own_q, across, hx_send, hx_recv).start()
            hid_copy(i, own_q, mate, hc_send, hc_recv).start()

        @pl.when(jnp.logical_and(s >= LAG_PASS, s < total_steps + LAG_PASS))
        def _():
            i = s - LAG_PASS
            hid_copy(i, far_q, across, hx_send, hx_recv).wait_recv()
            hid_copy(i, far_q, mate, hf_send, hf_recv).start()

        @pl.when(s >= LAG_DOWN)
        def _():
            i = s - LAG_DOWN
            hid_copy(i, own_q, mate, hc_send, hc_recv).wait_recv()
            hid_copy(i, far_q, mate, hf_send, hf_recv).wait_recv()
            value = acc[...]
            for q in range(4):
                value = value + jnp.dot(
                    hid[q, i],
                    down[pl.ds(pl.multiple_of(q * quarter + lax.rem(i, count) * CHUNK, CHUNK), CHUNK), :],
                    preferred_element_type=f32,
                )
            acc[...] = value

            @pl.when(i == count - 1)
            def _():
                outb[0] = acc[...].astype(bf16)
                ret_copy(1).start()
                acc[...] = jnp.zeros_like(acc)

        return carry

    lax.fori_loop(0, total_steps + LAG_DOWN, step, 0)

    outb[1] = acc[...].astype(bf16)
    for k in (2, 3):
        ret_copy(k).start()
    window = lax.broadcasted_iota(jnp.int32, (tok, WINDOW), 1).astype(f32)

    def returned(k):
        at_source = lanes == peers[k]
        shift = float((k % 2) * (CAP - CAP // ALIGN * ALIGN))
        place = jnp.sum(jnp.where(at_source, slot_all[0], 0.0), axis=1, keepdims=True) + shift
        chosen = jnp.where(place == window, 1.0, 0.0).astype(bf16)
        weight = jnp.sum(jnp.where(at_source, mix[...], 0.0), axis=1, keepdims=True)
        value = outb[0, 0:WINDOW, :] if k == 0 else ret[k]
        return weight * jnp.dot(chosen, value, preferred_element_type=f32)

    mixed = hkeep[...].astype(f32) + returned(0)
    for k in range(1, n_ep):
        ret_copy(k).wait_recv()
        mixed = mixed + returned(k)
    out_ref[...] = mixed.astype(bf16)
    for k in range(1, n_ep):
        ret_copy(k).wait_send()

    for copy in ctx_copies + slot_copies + part_copies + side_copies + x_copies + inv_copies:
        copy.wait_send()
    for copy, here in land_copies:

        @pl.when(jnp.logical_not(here))
        def _():
            copy.wait_send()

    def drain(i, carry):
        pair_copy(i).wait_send()
        far_copy(i).wait_send()
        hid_copy(i, own_q, across, hx_send, hx_recv).wait_send()
        hid_copy(i, own_q, mate, hc_send, hc_recv).wait_send()
        hid_copy(i, far_q, mate, hf_send, hf_recv).wait_send()
        return carry

    lax.fori_loop(0, total_steps, drain, 0)


def fused_device(context, stream, out_proj, norm_gain, router, expert_ids, w_gate, w_up, w_down):
    n_ep, n_tp = lax.axis_size("ep"), lax.axis_size("tp")
    tok, width = stream.shape
    heads = context.shape[1]
    hidden = w_gate.shape[1]
    cols = out_proj.shape[1]
    slots = 2 * CAP
    count = 2 * (hidden // n_tp // CHUNK)
    pieces = 4
    bf16, f32 = jnp.bfloat16, jnp.float32
    vmem, hbm = pl.BlockSpec(memory_space=pltpu.VMEM), pl.BlockSpec(memory_space=pl.ANY)
    dma = lambda n: pltpu.SemaphoreType.DMA((n,))
    scratch = [
        pltpu.VMEM(out_proj.shape, bf16),
        pltpu.VMEM(w_gate.shape, bf16),
        pltpu.VMEM(w_up.shape, bf16),
        pltpu.VMEM(w_down.shape, bf16),
        pltpu.VMEM((n_ep, tok, heads), bf16),
        pltpu.VMEM((n_ep, tok, cols), bf16),
        pltpu.VMEM((2, tok, cols), bf16),
        pltpu.VMEM((2, tok, cols), bf16),
        pltpu.VMEM((2, tok, cols), bf16),
        pltpu.VMEM((tok, width), bf16),
        pltpu.VMEM((n_ep, tok, width), bf16),
        pltpu.VMEM((2, slots, width), bf16),
        pltpu.VMEM((tok, 128), f32),
        pltpu.VMEM((n_tp - 1, tok, 128), f32),
        pltpu.VMEM((n_ep, tok, 128), f32),
        pltpu.VMEM((n_ep, tok, 128), f32),
        pltpu.VMEM((2, slots, 128), f32),
        pltpu.VMEM((2, slots, 2 * tok), f32),
        pltpu.VMEM((tok, 128), f32),
        pltpu.VMEM((count, 4, slots, CHUNK), bf16),
        pltpu.VMEM((count, 4, slots, CHUNK), bf16),
        pltpu.VMEM((2, 2, slots, CHUNK), f32),
        pltpu.VMEM((count, 2, slots, CHUNK), f32),
        pltpu.VMEM((count, 2, slots, CHUNK), bf16),
        pltpu.VMEM((count, 2, slots, CHUNK), bf16),
        pltpu.VMEM((4, count, slots, CHUNK), bf16),
        pltpu.VMEM((slots, width), f32),
        pltpu.VMEM((2, slots, width), bf16),
        pltpu.VMEM((n_ep, WINDOW, width), bf16),
        dma(4 * pieces),
    ]
    for size in (n_ep - 1, n_ep - 1, 2, 2, n_tp - 1, n_ep - 1, n_ep - 1, count, count, count, count, count, n_ep - 1):
        scratch += [dma(size), dma(size)]
    return pl.pallas_call(
        functools.partial(fused_kernel, n_ep, n_tp, pieces),
        out_shape=jax.ShapeDtypeStruct((tok, width), bf16),
        in_specs=[vmem] * 5 + [hbm] * 4,
        out_specs=vmem,
        scratch_shapes=scratch,
        compiler_params=pltpu.CompilerParams(
            collective_id=0, has_side_effects=True, vmem_limit_bytes=VMEM_BYTES
        ),
        name="fused_layer",
    )(context, stream, norm_gain, router.T, expert_ids.T, out_proj, w_gate, w_up, w_down)


def solution(mesh):
    sizes = dict(mesh.shape)
    fused = sizes["tp"] == 4 and sizes["ep"] == EXPERTS
    return jax.shard_map(
        fused_device if fused else plain_device,
        mesh=mesh,
        in_specs=(
            P(("groups", "ep"), "tp"),
            P(("groups", "ep"), "tp"),
            P("tp", "ep"),
            P("tp"),
            P("tp", None),
            P(("groups", "ep"), None),
            P("tp", "ep"),
            P("tp", "ep"),
            P("ep", "tp"),
        ),
        out_specs=P(("groups", "ep"), "tp"),
        check_vma=False,
    )
```

```python
import functools

import jax
import jax.numpy as jnp
from jax import lax
from jax.experimental import pallas as pl
from jax.experimental.pallas import tpu as pltpu
from jax.sharding import PartitionSpec as P

D = 4096
EXPERTS = 4
CAP = 36


def plain_device(context, stream, out_proj, norm_gain, router, expert_ids, w_gate, w_up, w_down):
    tok_rows = stream.shape[0]
    width_part = stream.shape[1]
    ep_count = lax.axis_size("ep")
    fanout = ep_count // EXPERTS
    columns = jnp.dot(
        lax.all_gather(context, "ep", axis=0, tiled=True),
        out_proj,
        preferred_element_type=jnp.float32,
    )
    head_part = lax.all_to_all(
        columns.astype(jnp.bfloat16), "ep", split_axis=0, concat_axis=1, tiled=True
    )
    attention = lax.psum_scatter(head_part, "tp", scatter_dimension=1, tiled=True).astype(
        jnp.float32
    )
    hstate = (stream.astype(jnp.float32) + attention).astype(jnp.bfloat16)
    hfloat = hstate.astype(jnp.float32)
    gain_vec = norm_gain.astype(jnp.float32)
    router_wide = router.astype(jnp.float32)
    squares = jnp.sum(hfloat * hfloat, axis=1)
    total_sq = lax.psum(squares, "tp")
    inverse = lax.rsqrt(total_sq / D + 1e-05)[:, None]
    normed = hfloat * inverse * gain_vec[None, :]
    logits = lax.psum(jnp.dot(normed, router_wide, precision=lax.Precision.HIGHEST), "tp")
    inputs = normed.astype(jnp.bfloat16)
    experts_range = jnp.arange(EXPERTS, dtype=jnp.int32)
    flat_ids = expert_ids.reshape(tok_rows * 2)
    onehot = (flat_ids[:, None] == experts_range[None, :]).astype(jnp.int32)
    before = jnp.cumsum(onehot, axis=0) - onehot
    slot_index = jnp.sum(before * onehot, axis=1)
    target = flat_ids * CAP + slot_index
    picked = onehot.reshape(tok_rows, 2, EXPERTS).astype(jnp.float32)
    chosen = jnp.sum(picked * logits[:, None, :], axis=2)
    leading = jax.nn.sigmoid(chosen[:, 0] - chosen[:, 1])
    weights = jnp.stack([leading, 1.0 - leading], axis=1)
    columns_all = jnp.arange(EXPERTS * CAP, dtype=jnp.int32)
    placement = (
        (target[:, None] == columns_all[None, :])
        .astype(jnp.float32)
        .reshape(tok_rows, 2, EXPERTS * CAP)
    )
    dispatch = jnp.sum(placement, axis=1)
    combine = jnp.sum(placement * weights[:, :, None], axis=1)
    sectioned = lax.dot_general(
        dispatch.astype(jnp.bfloat16),
        inputs,
        (((0,), (0,)), ((), ())),
        preferred_element_type=jnp.float32,
    ).astype(jnp.bfloat16)
    send_rows = jnp.broadcast_to(
        sectioned.reshape(EXPERTS, 1, CAP, width_part), (EXPERTS, fanout, CAP, width_part)
    ).reshape(ep_count, CAP, width_part)
    received = lax.all_to_all(send_rows, "ep", split_axis=0, concat_axis=0, tiled=True)
    slot_count = received.shape[1]
    flattened = received.reshape(ep_count * slot_count, width_part)
    gate_part = jnp.dot(flattened, w_gate, preferred_element_type=jnp.float32)
    up_part = jnp.dot(flattened, w_up, preferred_element_type=jnp.float32)
    gate_sum = lax.psum(gate_part.astype(jnp.bfloat16), "tp").astype(jnp.float32)
    up_sum = lax.psum(up_part.astype(jnp.bfloat16), "tp").astype(jnp.float32)
    hidden = (jax.nn.silu(gate_sum) * up_sum).astype(jnp.bfloat16)
    partial_value = jnp.dot(hidden, w_down, preferred_element_type=jnp.float32).astype(jnp.bfloat16)
    returned_rows = lax.all_to_all(
        partial_value.reshape(ep_count, slot_count, width_part),
        "ep",
        split_axis=0,
        concat_axis=0,
        tiled=True,
    )
    summed = jnp.sum(
        returned_rows.astype(jnp.float32).reshape(EXPERTS, fanout, CAP, width_part), axis=1
    ).reshape(EXPERTS * CAP, width_part)
    expert_mix = jnp.dot(combine, summed, precision=lax.Precision.HIGHEST)
    return (hfloat + expert_mix).astype(jnp.bfloat16)


MESH = pl.DeviceIdType.MESH
CHUNK = 256
LAG_SUM, LAG_PASS, LAG_DOWN = 4, 7, 9
WINDOW = 40
ALIGN = 8
VMEM_BYTES = 67043328


def fused_kernel(
    n_ep,
    n_tp,
    pieces,
    ctx_ref,
    stream_ref,
    gain_ref,
    router_ref,
    ids_ref,
    proj_hbm,
    gate_hbm,
    up_hbm,
    down_hbm,
    out_ref,
    proj,
    gate,
    up,
    down,
    ctx_all,
    part,
    part_in,
    halves,
    landed,
    hkeep,
    x_all,
    rows,
    side,
    side_all,
    inv_all,
    slot_all,
    inv_rows,
    chooser,
    mix,
    pair_out,
    pair_in,
    own_far,
    own_near,
    far_out,
    far_in,
    hid,
    acc,
    outb,
    ret,
    w_sem,
    ctx_send,
    ctx_recv,
    slot_send,
    slot_recv,
    part_send,
    part_recv,
    land_send,
    land_recv,
    side_send,
    side_recv,
    x_send,
    x_recv,
    inv_send,
    inv_recv,
    pair_send,
    pair_recv,
    far_send,
    far_recv,
    hx_send,
    hx_recv,
    hc_send,
    hc_recv,
    hf_send,
    hf_recv,
    ret_send,
    ret_recv,
):
    me = lax.axis_index("ep")
    lane = lax.axis_index("tp")
    core = lax.rem(lane, 2)
    side_x = lane // 2
    mate = 2 * side_x + (1 - core)
    across = 2 * (1 - side_x) + core
    tok, width = stream_ref.shape
    depth = n_tp * width
    quarter = gate.shape[1] // n_tp
    count = quarter // CHUNK
    total_steps = 2 * count
    slots = rows.shape[1]
    f32, bf16 = jnp.float32, jnp.bfloat16
    peers = (me, me + 1 - 2 * lax.rem(me, 2), lax.rem(me + 2, 4), 3 - me)

    loads = {}
    number = 0
    for name, src, dst in (("p", proj_hbm, proj), ("g", gate_hbm, gate), ("u", up_hbm, up), ("d", down_hbm, down)):
        step = src.shape[0] // pieces
        group = []
        for p in range(pieces):
            copy = pltpu.make_async_copy(
                src.at[pl.ds(p * step, step)], dst.at[pl.ds(p * step, step)], w_sem.at[number]
            )
            copy.start()
            group.append(copy)
            number += 1
        loads[name] = group

    barrier = pltpu.get_barrier_semaphore()
    for de in range(n_ep):
        for dt in range(n_tp):
            if de or dt:
                pl.semaphore_signal(
                    barrier,
                    inc=1,
                    device_id={"ep": lax.rem(me + de, n_ep), "tp": lax.rem(lane + dt, n_tp)},
                    device_id_type=MESH,
                )

    experts = lax.broadcasted_iota(jnp.int32, (128, tok), 0)
    is_first = jnp.transpose(jnp.where(ids_ref[0:1, :] == experts, 1.0, 0.0).astype(f32))
    is_second = jnp.transpose(jnp.where(ids_ref[1:2, :] == experts, 1.0, 0.0).astype(f32))
    named = is_first + is_second
    lanes = lax.broadcasted_iota(jnp.int32, (tok, 128), 1)
    row_i = lax.broadcasted_iota(jnp.int32, (tok, tok), 0)
    col_i = lax.broadcasted_iota(jnp.int32, (tok, tok), 1)
    lower = jnp.where(col_i < row_i, 1.0, 0.0).astype(bf16)
    rank = jnp.dot(lower, named.astype(bf16), preferred_element_type=f32)
    slot_all[0] = jnp.where(named > 0.5, rank, -4096.0)

    pl.semaphore_wait(barrier, n_ep * n_tp - 1)

    def over_ep(src, dst, sends, recvs):
        copies = []
        for k in range(1, n_ep):
            copy = pltpu.make_async_remote_copy(
                src_ref=src,
                dst_ref=dst.at[k],
                send_sem=sends.at[k - 1],
                recv_sem=recvs.at[k - 1],
                device_id={"ep": peers[k]},
                device_id_type=MESH,
            )
            copy.start()
            copies.append(copy)
        return copies

    ctx_copies = over_ep(ctx_ref, ctx_all, ctx_send, ctx_recv)
    slot_copies = over_ep(slot_all.at[0], slot_all, slot_send, slot_recv)

    for copy in loads["p"]:
        copy.wait()
    part_copies, land_copies = [], []
    for i in range(2):
        pair = me // 2 if i == 0 else 1 - me // 2
        for k in (2 * i, 2 * i + 1):
            if k:
                ctx_copies[k - 1].wait_recv()
                value = ctx_all[k]
            else:
                value = ctx_ref[...]
            part[peers[k]] = jnp.dot(value, proj[...], preferred_element_type=f32).astype(bf16)
        copy = pltpu.make_async_remote_copy(
            src_ref=part.at[2 * pair + (1 - core)],
            dst_ref=part_in.at[i],
            send_sem=part_send.at[i],
            recv_sem=part_recv.at[i],
            device_id={"tp": mate},
            device_id_type=MESH,
        )
        copy.start()
        part_copies.append(copy)
        block = 2 * pair + core
        copy.wait_recv()
        halves[i] = (part[block].astype(f32) + part_in[i].astype(f32)).astype(bf16)
        copy = pltpu.make_async_remote_copy(
            src_ref=halves.at[i],
            dst_ref=landed.at[side_x],
            send_sem=land_send.at[i],
            recv_sem=land_recv.at[side_x],
            device_id={"ep": block, "tp": me},
            device_id_type=MESH,
        )
        here = jnp.logical_and(block == me, me == lane)

        @pl.when(here)
        def _():
            landed[side_x] = halves[i]

        @pl.when(jnp.logical_not(here))
        def _():
            copy.start()

        land_copies.append((copy, here))

    for copy in slot_copies:
        copy.wait_recv()
    wide = lanes.astype(f32)
    for g in range(2):
        columns = []
        for p in range(2):
            picked = jnp.sum(jnp.where(lanes == me, slot_all[2 * g + p], 0.0), axis=1, keepdims=True)
            columns.append(jnp.where(picked + float(p * CAP) == wide, 1.0, 0.0).astype(f32))
        chooser[g] = jnp.transpose(jnp.concatenate(columns, axis=0))[:slots]

    for j in range(2):
        source = 2 * j + lax.rem(me, 2)
        mine = jnp.logical_and(me == lane, source == lane)

        @pl.when(jnp.logical_not(mine))
        def _():
            pltpu.make_async_remote_copy(
                src_ref=halves.at[0],
                dst_ref=landed.at[j],
                send_sem=land_send.at[0],
                recv_sem=land_recv.at[j],
                device_id={"tp": mate},
                device_id_type=MESH,
            ).wait_recv()

    attention = landed[0].astype(f32) + landed[1].astype(f32)
    hstate = (stream_ref[...].astype(f32) + attention).astype(bf16)
    hkeep[...] = hstate
    hfloat = hstate.astype(f32)
    scaled = hfloat * gain_ref[...].astype(f32).reshape(1, width)
    x_all[0] = scaled.astype(bf16)
    x_copies = over_ep(x_all.at[0], x_all, x_send, x_recv)

    side[...] = jnp.zeros_like(side)
    side[:, 0:EXPERTS] = lax.dot_general(
        scaled,
        router_ref[...].astype(f32),
        (((1,), (1,)), ((), ())),
        precision=lax.Precision.HIGHEST,
        preferred_element_type=f32,
    )
    side[:, EXPERTS : EXPERTS + 1] = jnp.sum(hfloat * hfloat, axis=1, keepdims=True)
    side_copies = []
    for k in range(1, n_tp):
        copy = pltpu.make_async_remote_copy(
            src_ref=side,
            dst_ref=side_all.at[k - 1],
            send_sem=side_send.at[k - 1],
            recv_sem=side_recv.at[k - 1],
            device_id={"tp": lax.rem(lane + k, n_tp)},
            device_id_type=MESH,
        )
        copy.start()
        side_copies.append(copy)
    total = side[...]
    for k in range(1, n_tp):
        side_copies[k - 1].wait_recv()
        total = total + side_all[k - 1]
    inverse = lax.rsqrt(total[:, EXPERTS : EXPERTS + 1] / depth + 1e-05)
    logits = total * inverse
    first = jnp.sum(is_first * logits, axis=1, keepdims=True)
    second = jnp.sum(is_second * logits, axis=1, keepdims=True)
    leading = jax.nn.sigmoid(first - second)
    mix[...] = is_first * leading + is_second * (1.0 - leading)
    inv_all[0] = jnp.broadcast_to(inverse, (tok, 128))
    inv_copies = over_ep(inv_all.at[0], inv_all, inv_send, inv_recv)

    def fill_rows(g):
        rows[g] = jnp.dot(
            chooser[g].astype(bf16),
            x_all[2 * g : 2 * g + 2].reshape(2 * tok, width),
            preferred_element_type=f32,
        ).astype(bf16)

    def fill_inverse(g):
        inv_rows[g] = jnp.dot(
            chooser[g],
            inv_all[2 * g : 2 * g + 2].reshape(2 * tok, 128),
            precision=lax.Precision.HIGHEST,
            preferred_element_type=f32,
        )

    acc[...] = jnp.zeros_like(acc)
    for name in ("g", "u", "d"):
        for copy in loads[name]:
            copy.wait()
    x_copies[0].wait_recv()
    fill_rows(0)

    def ret_copy(k):
        return pltpu.make_async_remote_copy(
            src_ref=outb.at[k // 2, pl.ds((k % 2) * (CAP // ALIGN * ALIGN), WINDOW)],
            dst_ref=ret.at[k],
            send_sem=ret_send.at[k - 1],
            recv_sem=ret_recv.at[k - 1],
            device_id={"ep": peers[k]},
            device_id_type=MESH,
        )

    def pair_copy(i):
        return pltpu.make_async_remote_copy(
            src_ref=pair_out.at[i], dst_ref=pair_in.at[i], send_sem=pair_send.at[i], recv_sem=pair_recv.at[i],
            device_id={"tp": mate}, device_id_type=MESH,
        )

    def far_copy(i):
        return pltpu.make_async_remote_copy(
            src_ref=far_out.at[i], dst_ref=far_in.at[i], send_sem=far_send.at[i], recv_sem=far_recv.at[i],
            device_id={"tp": across}, device_id_type=MESH,
        )

    own_q = 2 * core + side_x
    far_q = 2 * core + (1 - side_x)

    def hid_copy(i, q, target, sends, recvs):
        return pltpu.make_async_remote_copy(
            src_ref=hid.at[q, i], dst_ref=hid.at[q, i], send_sem=sends.at[i], recv_sem=recvs.at[i],
            device_id={"tp": target}, device_id_type=MESH,
        )

    def columns_of(weight, q, i):
        return weight[:, pl.ds(pl.multiple_of(q * quarter + lax.rem(i, count) * CHUNK, CHUNK), CHUNK)]

    def step(s, carry):
        @pl.when(s == count)
        def _():
            for k in (2, 3):
                x_copies[k - 1].wait_recv()
            fill_rows(1)

        @pl.when(s < total_steps)
        def _():
            i = s
            value = rows[i // count]
            for j in range(2):
                for m, weight in enumerate((gate, up)):
                    pair_out[i, 2 * j + m] = jnp.dot(
                        value, columns_of(weight, 2 * (1 - core) + j, i), preferred_element_type=f32
                    ).astype(bf16)
            pair_copy(i).start()
            for m, weight in enumerate((gate, up)):
                own_far[lax.rem(i, 2), m] = jnp.dot(
                    value, columns_of(weight, far_q, i), preferred_element_type=f32
                )
                own_near[i, m] = jnp.dot(
                    value, columns_of(weight, own_q, i), preferred_element_type=f32
                )

        @pl.when(jnp.logical_and(s >= 1, s < total_steps + 1))
        def _():
            i = s - 1
            pair_copy(i).wait_recv()
            for m in range(2):
                far_out[i, m] = (
                    own_far[lax.rem(i, 2), m] + pair_in[i, 2 * (1 - side_x) + m].astype(f32)
                ).astype(bf16)
            far_copy(i).start()
            for m in range(2):
                own_near[i, m] = own_near[i, m] + pair_in[i, 2 * side_x + m].astype(f32)

        @pl.when(s == LAG_SUM)
        def _():
            inv_copies[0].wait_recv()
            fill_inverse(0)

        @pl.when(s == count + LAG_SUM)
        def _():
            for k in (2, 3):
                inv_copies[k - 1].wait_recv()
            fill_inverse(1)

        @pl.when(jnp.logical_and(s >= LAG_SUM, s < total_steps + LAG_SUM))
        def _():
            i = s - LAG_SUM
            far_copy(i).wait_recv()
            scale = inv_rows[i // count, :, 0:1]
            g = (own_near[i, 0] + far_in[i, 0].astype(f32)) * scale
            u = (own_near[i, 1] + far_in[i, 1].astype(f32)) * scale
            hid[own_q, i] = (g / (1.0 + jnp.exp(-g)) * u).astype(bf16)
            hid_copy(i, own_q, across, hx_send, hx_recv).start()
            hid_copy(i, own_q, mate, hc_send, hc_recv).start()

        @pl.when(jnp.logical_and(s >= LAG_PASS, s < total_steps + LAG_PASS))
        def _():
            i = s - LAG_PASS
            hid_copy(i, far_q, across, hx_send, hx_recv).wait_recv()
            hid_copy(i, far_q, mate, hf_send, hf_recv).start()

        @pl.when(s >= LAG_DOWN)
        def _():
            i = s - LAG_DOWN
            hid_copy(i, own_q, mate, hc_send, hc_recv).wait_recv()
            hid_copy(i, far_q, mate, hf_send, hf_recv).wait_recv()
            value = acc[...]
            for q in range(4):
                value = value + jnp.dot(
                    hid[q, i],
                    down[pl.ds(pl.multiple_of(q * quarter + lax.rem(i, count) * CHUNK, CHUNK), CHUNK), :],
                    preferred_element_type=f32,
                )
            acc[...] = value

            @pl.when(i == count - 1)
            def _():
                outb[0] = acc[...].astype(bf16)
                ret_copy(1).start()
                acc[...] = jnp.zeros_like(acc)

        return carry

    lax.fori_loop(0, total_steps + LAG_DOWN, step, 0)

    outb[1] = acc[...].astype(bf16)
    for k in (2, 3):
        ret_copy(k).start()
    window = lax.broadcasted_iota(jnp.int32, (tok, WINDOW), 1).astype(f32)

    def returned(k):
        at_source = lanes == peers[k]
        shift = float((k % 2) * (CAP - CAP // ALIGN * ALIGN))
        place = jnp.sum(jnp.where(at_source, slot_all[0], 0.0), axis=1, keepdims=True) + shift
        chosen = jnp.where(place == window, 1.0, 0.0).astype(bf16)
        weight = jnp.sum(jnp.where(at_source, mix[...], 0.0), axis=1, keepdims=True)
        value = outb[0, 0:WINDOW, :] if k == 0 else ret[k]
        return weight * jnp.dot(chosen, value, preferred_element_type=f32)

    mixed = hkeep[...].astype(f32) + returned(0)
    for k in range(1, n_ep):
        ret_copy(k).wait_recv()
        mixed = mixed + returned(k)
    out_ref[...] = mixed.astype(bf16)
    for k in range(1, n_ep):
        ret_copy(k).wait_send()

    for copy in ctx_copies + slot_copies + part_copies + side_copies + x_copies + inv_copies:
        copy.wait_send()
    for copy, here in land_copies:

        @pl.when(jnp.logical_not(here))
        def _():
            copy.wait_send()

    def drain(i, carry):
        pair_copy(i).wait_send()
        far_copy(i).wait_send()
        hid_copy(i, own_q, across, hx_send, hx_recv).wait_send()
        hid_copy(i, own_q, mate, hc_send, hc_recv).wait_send()
        hid_copy(i, far_q, mate, hf_send, hf_recv).wait_send()
        return carry

    lax.fori_loop(0, total_steps, drain, 0)


def fused_device(context, stream, out_proj, norm_gain, router, expert_ids, w_gate, w_up, w_down):
    n_ep, n_tp = lax.axis_size("ep"), lax.axis_size("tp")
    tok, width = stream.shape
    heads = context.shape[1]
    hidden = w_gate.shape[1]
    cols = out_proj.shape[1]
    slots = 2 * CAP
    count = 2 * (hidden // n_tp // CHUNK)
    pieces = 4
    bf16, f32 = jnp.bfloat16, jnp.float32
    vmem, hbm = pl.BlockSpec(memory_space=pltpu.VMEM), pl.BlockSpec(memory_space=pl.ANY)
    dma = lambda n: pltpu.SemaphoreType.DMA((n,))
    scratch = [
        pltpu.VMEM(out_proj.shape, bf16),
        pltpu.VMEM(w_gate.shape, bf16),
        pltpu.VMEM(w_up.shape, bf16),
        pltpu.VMEM(w_down.shape, bf16),
        pltpu.VMEM((n_ep, tok, heads), bf16),
        pltpu.VMEM((n_ep, tok, cols), bf16),
        pltpu.VMEM((2, tok, cols), bf16),
        pltpu.VMEM((2, tok, cols), bf16),
        pltpu.VMEM((2, tok, cols), bf16),
        pltpu.VMEM((tok, width), bf16),
        pltpu.VMEM((n_ep, tok, width), bf16),
        pltpu.VMEM((2, slots, width), bf16),
        pltpu.VMEM((tok, 128), f32),
        pltpu.VMEM((n_tp - 1, tok, 128), f32),
        pltpu.VMEM((n_ep, tok, 128), f32),
        pltpu.VMEM((n_ep, tok, 128), f32),
        pltpu.VMEM((2, slots, 128), f32),
        pltpu.VMEM((2, slots, 2 * tok), f32),
        pltpu.VMEM((tok, 128), f32),
        pltpu.VMEM((count, 4, slots, CHUNK), bf16),
        pltpu.VMEM((count, 4, slots, CHUNK), bf16),
        pltpu.VMEM((2, 2, slots, CHUNK), f32),
        pltpu.VMEM((count, 2, slots, CHUNK), f32),
        pltpu.VMEM((count, 2, slots, CHUNK), bf16),
        pltpu.VMEM((count, 2, slots, CHUNK), bf16),
        pltpu.VMEM((4, count, slots, CHUNK), bf16),
        pltpu.VMEM((slots, width), f32),
        pltpu.VMEM((2, slots, width), bf16),
        pltpu.VMEM((n_ep, WINDOW, width), bf16),
        dma(4 * pieces),
    ]
    for size in (n_ep - 1, n_ep - 1, 2, 2, n_tp - 1, n_ep - 1, n_ep - 1, count, count, count, count, count, n_ep - 1):
        scratch += [dma(size), dma(size)]
    return pl.pallas_call(
        functools.partial(fused_kernel, n_ep, n_tp, pieces),
        out_shape=jax.ShapeDtypeStruct((tok, width), bf16),
        in_specs=[vmem] * 5 + [hbm] * 4,
        out_specs=vmem,
        scratch_shapes=scratch,
        compiler_params=pltpu.CompilerParams(
            collective_id=0, has_side_effects=True, vmem_limit_bytes=VMEM_BYTES
        ),
        name="fused_layer",
    )(context, stream, norm_gain, router.T, expert_ids.T, out_proj, w_gate, w_up, w_down)


def solution(mesh):
    sizes = dict(mesh.shape)
    fused = sizes["tp"] == 4 and sizes["ep"] == EXPERTS
    return jax.shard_map(
        fused_device if fused else plain_device,
        mesh=mesh,
        in_specs=(
            P(("groups", "ep"), "tp"),
            P(("groups", "ep"), "tp"),
            P("tp", "ep"),
            P("tp"),
            P("tp", None),
            P(("groups", "ep"), None),
            P("tp", "ep"),
            P("tp", "ep"),
            P("ep", "tp"),
        ),
        out_specs=P(("groups", "ep"), "tp"),
        check_vma=False,
    )
```
